32 devices in a mesh: samp: 4 (over z), seq: 8 (over y, x, core).
Axes of the slice: x: 2, y: 2, z: 4, core: 2. Of those that a mesh axis runs over, the one named last changes fastest.
Arguments:
- queries: bfloat16 [4, 4096, 3584], P('samp', 'seq'), may hold values from -200 to 200
- keys: bfloat16 [4, 4096, 512], P('samp', 'seq'), may hold values from -6 to 6
- values: bfloat16 [4, 4096, 512], P('samp', 'seq'), may hold values from -6 to 6
- reg_owner: int32 [4], P('samp'), may hold values from 0 to 7
- block_lists: int32 [4, 32, 8], P('samp', 'seq'), may hold values from 0 to 31, as said below
- list_counts: int32 [4, 32], P('samp', 'seq'), may hold values from 0 to 8, as said below
- image_blocks: int32 [4, 32], P('samp', 'seq'), may hold values from 0 to 1, as said below
Outputs:
- attended: bfloat16 [4, 4096, 3584], P('samp', 'seq')
The draws below stay inside these ranges and needn't reach their ends.
Inputs may be any that keep to these rules, and one draw needn't show every extreme that they name: `block_lists`: block b lies on sequence index b // 4. Entry t of a list is used only where t < the block's count, unused entries are 0. The used entries of one block name blocks of distinct sequence indices other than its own. Over all blocks of one sequence index, at most one distinct block of each other sequence index is named. On the last sequence index of each sample, the lists together name a block of every other index. `list_counts`: 0 for image blocks; at most 8. `image_blocks`: the blocks of the last sequence index of each sample are text blocks.
All inputs are finite; a program needn't handle non-finite values.
Results may differ from the reference program's by a relative error of at most 0.0043.
Values may be sent and summed in bfloat16 or wider, within the bound.
A program may use at most 128 MiB of HBM per device.

```python
import math
import jax
import jax.numpy as jnp
from jax import lax

QUERY_HEADS = 28
KEY_VALUE_HEADS = 4
HEAD_SIZE = 128
BLOCK_TOKENS = 128
REG = 64
LIST_ENTRIES = 8
BLK_DEV = 4
SAMPLE_COUNT = 4
TOK_DEV = 512
SAMPLE_BLOCKS = 32
SAMPLE_TOKENS = 4096
N_SEQ = 8


def activations(key):
    seeded = jax.random.fold_in(key, 11)
    key_queries, keys_for_keys = jax.random.split(seeded, 2)
    key_region = jnp.clip(jax.random.normal(keys_for_keys, (SAMPLE_COUNT, SAMPLE_TOKENS, KEY_VALUE_HEADS, HEAD_SIZE), jnp.float32), -6.0, 6.0)
    query_field = jnp.clip(jax.random.normal(key_queries, (SAMPLE_COUNT, SAMPLE_TOKENS, QUERY_HEADS, HEAD_SIZE), jnp.float32), -6.0, 6.0)
    query_out = query_field.reshape(SAMPLE_COUNT, SAMPLE_TOKENS, QUERY_HEADS * HEAD_SIZE).astype(jnp.bfloat16)
    key_output = key_region.reshape(SAMPLE_COUNT, SAMPLE_TOKENS, KEY_VALUE_HEADS * HEAD_SIZE).astype(jnp.bfloat16)
    return (query_out, key_output)


def draw_queries(key, part):
    return activations(key)[0]


def draw_keys(key, part):
    return activations(key)[1]


def layout(key):
    seeded = jax.random.fold_in(key, 7)
    key_kinds, key_chosen, key_order, key_counts = jax.random.split(seeded, 4)
    block_ids = jnp.arange(SAMPLE_BLOCKS, dtype=jnp.int32)
    block_device = block_ids // BLK_DEV
    local_ids = block_ids % BLK_DEV
    last_device = N_SEQ - 1
    kinds = (jax.random.randint(key_kinds, (SAMPLE_COUNT, SAMPLE_BLOCKS), 0, 4, jnp.int32) == 0).astype(jnp.int32)
    kinds = jnp.where(block_device[None, :] == last_device, 0, kinds)
    chosen = jax.random.randint(key_chosen, (SAMPLE_COUNT, N_SEQ, N_SEQ), 0, BLK_DEV, jnp.int32)
    owner_ids = jnp.arange(N_SEQ, dtype=jnp.int32)
    ranking = jax.random.randint(key_order, (SAMPLE_COUNT, SAMPLE_BLOCKS, N_SEQ), 0, 2 ** 16, jnp.int32) * N_SEQ + owner_ids
    ranking = jnp.where(owner_ids[None, None, :] != block_device[None, :, None], ranking, 2 ** 30)
    ordered = jnp.argsort(ranking, axis=-1)[..., :LIST_ENTRIES].astype(jnp.int32)
    slot_ids = jnp.arange(LIST_ENTRIES, dtype=jnp.int32)
    full_count = min(LIST_ENTRIES, N_SEQ - 1)
    cyclic = (local_ids[:, None] * full_count + slot_ids[None, :]) % (N_SEQ - 1)
    is_last = block_device == last_device
    ordered = jnp.where(is_last[None, :, None], cyclic[None], ordered)
    counts = full_count - jax.random.randint(key_counts, (SAMPLE_COUNT, SAMPLE_BLOCKS), 0, 3, jnp.int32)
    counts = jnp.where(is_last[None, :], full_count, counts)
    counts = jnp.where(kinds == 1, 0, counts)
    chosen_rows = chosen[:, block_device, :]
    picked = jnp.take_along_axis(chosen_rows, ordered, axis=2)
    list_ids = ordered * BLK_DEV + picked
    list_ids = jnp.where(slot_ids[None, None, :] < counts[..., None], list_ids, 0)
    return (list_ids.astype(jnp.int32), counts.astype(jnp.int32), kinds.astype(jnp.int32))


def draw_block_lists(key, part):
    return layout(key)[0]


def draw_list_counts(key, part):
    return layout(key)[1]


def draw_image_blocks(key, part):
    return layout(key)[2]


def place_ends(result, key, smallest, high):
    index_at = [jax.random.randint(jax.random.fold_in(key, axis), (), 0, length) for axis, length in enumerate(result.shape)]
    widest = result.shape.index(max(result.shape))
    beside = index_at[:widest] + [(index_at[widest] + 1) % result.shape[widest]] + index_at[widest + 1:]
    return result.at[tuple(index_at)].set(smallest).at[tuple(beside)].set(high)


def shard_levels(own_key, shape, cuts, low, high):
    gain = 1.0
    for dim, blocks in cuts:
        heights = jax.random.uniform(jax.random.fold_in(jax.random.fold_in(own_key, 6), dim), (blocks,), jnp.float32, low / len(cuts), high / len(cuts))
        gain = gain * jnp.repeat(jnp.exp(heights), shape[dim] // blocks).reshape((-1,) + (1,) * (len(shape) - 1 - dim))
    return gain


def normal_values(key, extent, width, most, pieces=(), kind=jnp.bfloat16):
    drawn = width * jax.random.normal(key, extent, jnp.float32)
    if pieces:
        drawn = drawn * shard_levels(key, extent, pieces, -0.22, 0.18)
    return jnp.clip(drawn, -most, most).astype(kind)


def setup_inputs(seed: int = 0) -> dict:
    splits = jax.random.split(jax.random.key(seed), 8)
    return {
        "queries": draw_queries(jax.random.fold_in(splits[7], 71), 0),
        "keys": draw_keys(jax.random.fold_in(splits[7], 71), 0),
        "values": normal_values(splits[2], (SAMPLE_COUNT, SAMPLE_TOKENS, KEY_VALUE_HEADS * HEAD_SIZE), 1.0, 6.0, ((0, 4), (1, 8))),
        "reg_owner": place_ends(jax.random.randint(splits[3], (SAMPLE_COUNT,), 0, N_SEQ), jax.random.fold_in(splits[3], 1), 0, N_SEQ - 1).astype(jnp.int32),
        "block_lists": draw_block_lists(jax.random.fold_in(splits[7], 71), 0),
        "list_counts": draw_list_counts(jax.random.fold_in(splits[7], 71), 0),
        "image_blocks": draw_image_blocks(jax.random.fold_in(splits[7], 71), 0),
    }


very_low = -1e+30

def group_part(query_row_list, key_row_list, value_row_list, visible):
    head_grouped = query_row_list.astype(jnp.float32).reshape(BLOCK_TOKENS, KEY_VALUE_HEADS, QUERY_HEADS // KEY_VALUE_HEADS, HEAD_SIZE)
    per_head_keys = key_row_list.astype(jnp.float32).reshape(-1, KEY_VALUE_HEADS, HEAD_SIZE)
    per_head_values = value_row_list.astype(jnp.float32).reshape(-1, KEY_VALUE_HEADS, HEAD_SIZE)
    scores = jnp.einsum('qhgd,khd->hgqk', head_grouped, per_head_keys) / math.sqrt(HEAD_SIZE)
    scores = jnp.where(visible, scores, very_low)
    maxima = lax.optimization_barrier(jnp.max(scores, axis=-1))
    weights = jnp.where(visible, jnp.exp(scores - maxima[..., None]), 0.0)
    totals = lax.optimization_barrier(jnp.sum(weights, axis=-1))
    rounded = lax.optimization_barrier(weights.astype(jnp.bfloat16)).astype(jnp.float32)
    partial_value = jnp.einsum('hgqk,khd->hgqd', rounded, per_head_values)
    return (maxima, totals, partial_value)

def combine(parts):
    top_score = jnp.maximum(jnp.maximum(parts[0][0], parts[1][0]), parts[2][0])
    numerator = jnp.zeros(parts[0][2].shape, jnp.float32)
    denominator = jnp.zeros(parts[0][1].shape, jnp.float32)
    for maxima, totals, partial_value in parts:
        rescale = jnp.exp(maxima - top_score)
        numerator = numerator + rescale[..., None] * partial_value
        denominator = denominator + rescale * totals
    merged = numerator / denominator[..., None]
    return merged.transpose(2, 0, 1, 3).reshape(merged.shape[2], -1)

def reference(queries, keys, values, reg_owner, block_lists, list_counts, image_blocks):
    outputs = []
    row_ids = jnp.arange(BLOCK_TOKENS)
    slot_rows = jnp.arange(LIST_ENTRIES * BLOCK_TOKENS) // BLOCK_TOKENS
    for sample in range(SAMPLE_COUNT):
        query_all = queries[sample]
        every_key = keys[sample]
        every_value = values[sample]
        blocked_keys = every_key.reshape(SAMPLE_BLOCKS, BLOCK_TOKENS, KEY_VALUE_HEADS * HEAD_SIZE)
        blocked_values = every_value.reshape(SAMPLE_BLOCKS, BLOCK_TOKENS, KEY_VALUE_HEADS * HEAD_SIZE)
        reg_start = (reg_owner[sample] * TOK_DEV).astype(jnp.int32)
        reg_keys = lax.dynamic_slice_in_dim(every_key, reg_start, REG, 0)
        reg_values = lax.dynamic_slice_in_dim(every_value, reg_start, REG, 0)
        sample_lists = block_lists[sample]
        sample_counts = list_counts[sample]
        sample_image = image_blocks[sample]

        def one_block(block_id):
            row_start = (block_id * BLOCK_TOKENS).astype(jnp.int32)
            query_row_list = lax.dynamic_slice_in_dim(query_all, row_start, BLOCK_TOKENS, 0)
            own_keys = lax.dynamic_slice_in_dim(every_key, row_start, BLOCK_TOKENS, 0)
            own_values = lax.dynamic_slice_in_dim(every_value, row_start, BLOCK_TOKENS, 0)
            listed_block_index = sample_lists[block_id]
            remote_keys = blocked_keys[listed_block_index].reshape(LIST_ENTRIES * BLOCK_TOKENS, KEY_VALUE_HEADS * HEAD_SIZE)
            remote_values = blocked_values[listed_block_index].reshape(LIST_ENTRIES * BLOCK_TOKENS, KEY_VALUE_HEADS * HEAD_SIZE)
            reg_visible = jnp.ones((BLOCK_TOKENS, REG), bool)
            own_visible = (row_ids[None, :] <= row_ids[:, None]) | (sample_image[block_id] == 1)
            far_visible = jnp.broadcast_to(slot_rows[None, :] < sample_counts[block_id], (BLOCK_TOKENS, LIST_ENTRIES * BLOCK_TOKENS))
            parts = [group_part(query_row_list, reg_keys, reg_values, reg_visible), group_part(query_row_list, own_keys, own_values, own_visible), group_part(query_row_list, remote_keys, remote_values, far_visible)]
            return combine(parts).astype(jnp.bfloat16)
        blocks_out = lax.map(one_block, jnp.arange(SAMPLE_BLOCKS, dtype=jnp.int32))
        outputs.append(blocks_out.reshape(SAMPLE_TOKENS, QUERY_HEADS * HEAD_SIZE))
    return jnp.stack(outputs)
```

```python
import functools
import math

import jax
import jax.numpy as jnp
from jax import lax
from jax.experimental import pallas as pl
from jax.experimental.pallas import tpu as pltpu
from jax.sharding import PartitionSpec as P

KEY_VALUE_HEADS = 4
HEAD_SIZE = 128
REG = 64
CHUNKS = 8

hidden = -1e30
score_gain = math.log2(math.e) / math.sqrt(HEAD_SIZE)


def pair_order(devices):
    if devices == 8:
        return [(2, 4), (3, 5), (6, 7)]
    rest = list(range(2, devices))
    return [tuple(rest[i : i + 2]) for i in range(0, len(rest), 2)]


def kernel(
    devices,
    lists_ref,
    counts_ref,
    image_ref,
    owner_ref,
    q_hbm,
    k_hbm,
    v_hbm,
    out_ref,
    q_all,
    k_all,
    v_all,
    need_out,
    need_in,
    chunk_out,
    chunk_in,
    reg_out,
    reg_in,
    x_out,
    x_in,
    acc,
    top,
    bias,
    local_sem,
    q_sem,
    send_need,
    recv_need,
    send_chunk,
    recv_chunk,
    send_reg,
    recv_reg,
    send_x,
    recv_x,
):
    me = lax.axis_index("seq")
    blocks, slots = lists_ref.shape
    rows = k_hbm.shape[1]
    heads = q_hbm.shape[1] // HEAD_SIZE
    group = heads // KEY_VALUE_HEADS
    chunk_rows = 2 * REG // CHUNKS
    peers = range(1, devices)

    def peer(k):
        return me ^ k

    barrier = pltpu.get_barrier_semaphore()
    for k in peers:
        pl.semaphore_signal(barrier, inc=1, device_id={"seq": peer(k)})
    k_copy = pltpu.make_async_copy(k_hbm, k_all, local_sem.at[0])
    v_copy = pltpu.make_async_copy(v_hbm, v_all, local_sem.at[1])
    k_copy.start()
    v_copy.start()

    def q_copy(b):
        span = pl.ds(pl.multiple_of(b * rows, rows), rows)
        return pltpu.make_async_copy(q_hbm.at[span], q_all.at[span], q_sem.at[b])

    for b in range(blocks):
        q_copy(b).start()

    lane = lax.broadcasted_iota(jnp.int32, (8, 128), 1)
    wanted = jnp.zeros((8, 128), jnp.int32)
    for b in range(blocks):
        count = counts_ref[b]
        for t in range(slots):
            entry = lists_ref[b, t]
            source = jnp.where(t < count, lax.div(entry, blocks), -1)
            wanted = jnp.where(lane == source, lax.rem(entry, blocks), wanted)
    need_out[...] = wanted
    k_copy.wait()
    v_copy.wait()
    for c in range(CHUNKS):
        whole = k_all if c < CHUNKS // 2 else v_all
        start = (c % (CHUNKS // 2)) * chunk_rows
        chunk_out[c] = whole[0, start : start + chunk_rows]
    pl.semaphore_wait(barrier, devices - 1)

    def need_copy(k):
        return pltpu.make_async_remote_copy(
            need_out, need_in.at[k], send_need.at[k], recv_need.at[k], device_id={"seq": peer(k)}
        )

    def chunk_copy(k):
        return pltpu.make_async_remote_copy(
            chunk_out.at[lax.rem(peer(k), CHUNKS)],
            chunk_in.at[me],
            send_chunk.at[k],
            recv_chunk.at[k],
            device_id={"seq": peer(k)},
        )

    def reg_copy(k):
        return pltpu.make_async_remote_copy(
            reg_out, reg_in.at[me], send_reg.at[k], recv_reg.at[k], device_id={"seq": peer(k)}
        )

    def x_copy(k, g):
        return pltpu.make_async_remote_copy(
            x_out.at[k, g], x_in.at[k, g], send_x.at[k, g], recv_x.at[k, g], device_id={"seq": peer(k)}
        )

    order = list(reversed(peers))
    for k in order:
        need_copy(k).start()
    for k in order:
        chunk_copy(k).start()
    chunk_in[me] = chunk_out[lax.rem(me, CHUNKS)]

    for b in range(blocks):
        count = counts_ref[b]
        for k in peers:
            source = peer(k)
            seen = jnp.int32(0)
            for t in range(slots):
                entry = lists_ref[b, t]
                hit = jnp.logical_and(lax.div(entry, blocks) == source, t < count)
                seen = jnp.where(hit, 1, seen)
            bias[b, k] = jnp.where(seen == 1, 0.0, hidden)

    pairs = pair_order(devices)
    sends = [(1,)] + pairs

    for k in peers:
        need_copy(k).wait_recv()
    for group_of in sends:
        for k in group_of:
            row = need_in[k]
            pick = jnp.sum(jnp.where(lane[:1] == me, row[:1], 0))
            k_block = k_all[pick]
            v_block = v_all[pick]
            for g in range(KEY_VALUE_HEADS):
                columns = slice(g * HEAD_SIZE, (g + 1) * HEAD_SIZE)
                x_out[k, g, :rows] = k_block[:, columns]
                x_out[k, g, rows:] = v_block[:, columns]
        for g in range(KEY_VALUE_HEADS):
            for k in group_of:
                x_copy(k, g).start()

    for k in peers:
        chunk_copy(k).wait_recv()
    mine = chunk_in[owner_ref[0]]
    reg_out[...] = mine
    reg_in[me] = mine
    for k in order:
        reg_copy(k).start()

    def attend(b, g, keys, values, masks, first, last):
        index = g * blocks + b
        row_span = pl.ds(pl.multiple_of(b * rows, rows), rows)
        ones = jnp.ones(values.shape, values.dtype)
        wide = jnp.concatenate([values, ones], axis=1)
        for h in range(group):
            column = pl.ds(pl.multiple_of((g * group + h) * HEAD_SIZE, HEAD_SIZE), HEAD_SIZE)
            here = pl.ds(h * rows, rows)
            query = q_all[row_span, column]
            scores = lax.dot_general(
                query, keys, (((1,), (1,)), ((), ())), preferred_element_type=jnp.float32
            )
            scores = scores * score_gain + masks
            best = jnp.max(scores, axis=1, keepdims=True)
            if first:
                best = jnp.broadcast_to(best, (rows, 128))
            else:
                before = top[index, here]
                best = jnp.maximum(before, best)
            if scores.shape[1] > 128:
                spread = jnp.concatenate([best] * (scores.shape[1] // 128), axis=1)
            else:
                spread = best
            weights = jnp.exp2(scores - spread).astype(jnp.bfloat16)
            product = jnp.dot(weights, wide, preferred_element_type=jnp.float32)
            if not first:
                scale = jnp.exp2(before - best)
                product = product + acc[index, here] * jnp.concatenate([scale, scale], axis=1)
            if last:
                merged = product[:, :HEAD_SIZE] / product[:, HEAD_SIZE:]
                out_ref[row_span, column] = merged.astype(out_ref.dtype)
            else:
                acc[index, here] = product
                top[index, here] = best

    def own_step(i, carry):
        b = i // KEY_VALUE_HEADS
        g = lax.rem(i, KEY_VALUE_HEADS)

        @pl.when(g == 0)
        def _():
            q_copy(b).wait()

        column = pl.ds(pl.multiple_of(g * HEAD_SIZE, HEAD_SIZE), HEAD_SIZE)
        below = lax.broadcasted_iota(jnp.int32, (rows, rows), 1) <= lax.broadcasted_iota(
            jnp.int32, (rows, rows), 0
        )
        shut = jnp.where(image_ref[b] == 1, 0.0, hidden)
        masks = jnp.where(below, 0.0, shut)
        attend(b, g, k_all[b, :, column], v_all[b, :, column], masks, True, False)
        return carry

    lax.fori_loop(0, blocks * KEY_VALUE_HEADS, own_step, 0)

    for k in peers:
        reg_copy(k).wait_recv()

    side = lax.broadcasted_iota(jnp.int32, (1, 256), 1)
    half = CHUNKS // 2

    def reg_step(i, carry):
        g = i // blocks
        b = lax.rem(i, blocks)

        @pl.when(b == 0)
        def _():
            x_copy(1, g).wait_recv()

        column = pl.ds(pl.multiple_of(g * HEAD_SIZE, HEAD_SIZE), HEAD_SIZE)
        fill = jnp.zeros((REG, HEAD_SIZE), jnp.bfloat16)
        reg_keys = reg_in[pl.ds(0, half), :, column].reshape(REG, HEAD_SIZE)
        reg_values = reg_in[pl.ds(half, half), :, column].reshape(REG, HEAD_SIZE)
        keys = jnp.concatenate([x_in[1, g, :rows], reg_keys, fill], axis=0)
        values = jnp.concatenate([x_in[1, g, rows:], reg_values, fill], axis=0)
        masks = jnp.where(side < rows, bias[b, 1], jnp.where(side < rows + REG, 0.0, hidden))
        attend(b, g, keys, values, masks, False, False)
        return carry

    lax.fori_loop(0, blocks * KEY_VALUE_HEADS, reg_step, 0)

    for pair in pairs:

        def far_step(i, carry, pair=pair):
            g = i // blocks
            b = lax.rem(i, blocks)

            @pl.when(b == 0)
            def _():
                for k in pair:
                    x_copy(k, g).wait_recv()

            keys = jnp.concatenate([x_in[k, g, :rows] for k in pair], axis=0)
            values = jnp.concatenate([x_in[k, g, rows:] for k in pair], axis=0)
            masks = jnp.where(side < rows, bias[b, pair[0]], bias[b, pair[-1]])
            attend(b, g, keys, values, masks, False, pair == pairs[-1])
            return carry

        lax.fori_loop(0, blocks * KEY_VALUE_HEADS, far_step, 0)

    for k in peers:
        need_copy(k).wait_send()
        chunk_copy(k).wait_send()
        reg_copy(k).wait_send()
        for g in range(KEY_VALUE_HEADS):
            x_copy(k, g).wait_send()


def per_device(queries, keys, values, reg_owner, block_lists, list_counts, image_blocks):
    devices = lax.axis_size("seq")
    tokens, width = queries.shape[1:]
    kv_width = keys.shape[2]
    blocks = block_lists.shape[1]
    rows = tokens // blocks
    chunk_rows = 2 * REG // CHUNKS
    group_rows = width // kv_width * rows
    bf = jnp.bfloat16
    dma = pltpu.SemaphoreType.DMA
    smem = pl.BlockSpec(memory_space=pltpu.SMEM)
    anywhere = pl.BlockSpec(memory_space=pl.ANY)
    out = pl.pallas_call(
        functools.partial(kernel, devices),
        out_shape=jax.ShapeDtypeStruct((tokens, width), bf),
        in_specs=[smem] * 4 + [anywhere] * 3,
        out_specs=pl.BlockSpec(memory_space=pltpu.VMEM),
        scratch_shapes=[
            pltpu.VMEM((tokens, width), bf),
            pltpu.VMEM((blocks, rows, kv_width), bf),
            pltpu.VMEM((blocks, rows, kv_width), bf),
            pltpu.VMEM((8, 128), jnp.int32),
            pltpu.VMEM((devices, 8, 128), jnp.int32),
            pltpu.VMEM((CHUNKS, chunk_rows, kv_width), bf),
            pltpu.VMEM((devices, chunk_rows, kv_width), bf),
            pltpu.VMEM((chunk_rows, kv_width), bf),
            pltpu.VMEM((devices, chunk_rows, kv_width), bf),
            pltpu.VMEM((devices, KEY_VALUE_HEADS, 2 * rows, HEAD_SIZE), bf),
            pltpu.VMEM((devices, KEY_VALUE_HEADS, 2 * rows, HEAD_SIZE), bf),
            pltpu.VMEM((blocks * KEY_VALUE_HEADS, group_rows, 2 * HEAD_SIZE), jnp.float32),
            pltpu.VMEM((blocks * KEY_VALUE_HEADS, group_rows, 128), jnp.float32),
            pltpu.SMEM((blocks, devices), jnp.float32),
            dma((2,)),
            dma((blocks,)),
            dma((devices,)),
            dma((devices,)),
            dma((devices,)),
            dma((devices,)),
            dma((devices,)),
            dma((devices,)),
            dma((devices, KEY_VALUE_HEADS)),
            dma((devices, KEY_VALUE_HEADS)),
        ],
        compiler_params=pltpu.CompilerParams(
            collective_id=0, has_side_effects=True, vmem_limit_bytes=56 * 1024 * 1024
        ),
    )(
        block_lists[0],
        list_counts[0],
        image_blocks[0],
        reg_owner,
        queries[0],
        keys.reshape(blocks, rows, kv_width),
        values.reshape(blocks, rows, kv_width),
    )
    return out[None]


def solution(mesh):
    placed = (
        P("samp", "seq", None),
        P("samp", "seq", None),
        P("samp", "seq", None),
        P("samp"),
        P("samp", "seq", None),
        P("samp", "seq"),
        P("samp", "seq"),
    )
    return jax.shard_map(
        per_device, mesh=mesh, in_specs=placed, out_specs=P("samp", "seq", None), check_vma=False
    )
```

```python
import functools
import math

import jax
import jax.numpy as jnp
from jax import lax
from jax.experimental import pallas as pl
from jax.experimental.pallas import tpu as pltpu
from jax.sharding import PartitionSpec as P

KEY_VALUE_HEADS = 4
HEAD_SIZE = 128
REG = 64
CHUNKS = 8

hidden = -1e30
score_gain = math.log2(math.e) / math.sqrt(HEAD_SIZE)


def stage_list(devices):
    if devices == 8:
        return [(1, 2, 4, 3, 5, 6, 7)]
    rest = list(range(1, devices))
    return [tuple(rest[i : i + 7]) for i in range(0, len(rest), 7)]


def kernel(
    devices,
    lists_ref,
    counts_ref,
    image_ref,
    owner_ref,
    q_hbm,
    k_hbm,
    v_hbm,
    out_ref,
    q_all,
    k_all,
    v_all,
    need_out,
    need_in,
    chunk_out,
    chunk_in,
    reg_out,
    reg_in,
    x_out,
    x_in,
    acc,
    top,
    bias,
    local_sem,
    q_sem,
    send_need,
    recv_need,
    send_chunk,
    recv_chunk,
    send_reg,
    recv_reg,
    send_x,
    recv_x,
):
    me = lax.axis_index("seq")
    blocks, slots = lists_ref.shape
    rows = k_hbm.shape[1]
    heads = q_hbm.shape[1] // HEAD_SIZE
    group = heads // KEY_VALUE_HEADS
    chunk_rows = 2 * REG // CHUNKS
    peers = range(1, devices)

    def peer(k):
        return me ^ k

    barrier = pltpu.get_barrier_semaphore()
    for k in peers:
        pl.semaphore_signal(barrier, inc=1, device_id={"seq": peer(k)})
    k_copy = pltpu.make_async_copy(k_hbm, k_all, local_sem.at[0])
    v_copy = pltpu.make_async_copy(v_hbm, v_all, local_sem.at[1])
    k_copy.start()
    v_copy.start()

    def q_copy(b):
        span = pl.ds(pl.multiple_of(b * rows, rows), rows)
        return pltpu.make_async_copy(q_hbm.at[span], q_all.at[span], q_sem.at[b])

    for b in range(blocks):
        q_copy(b).start()

    lane = lax.broadcasted_iota(jnp.int32, (8, 128), 1)
    wanted = jnp.zeros((8, 128), jnp.int32)
    for b in range(blocks):
        count = counts_ref[b]
        for t in range(slots):
            entry = lists_ref[b, t]
            source = jnp.where(t < count, lax.div(entry, blocks), -1)
            wanted = jnp.where(lane == source, lax.rem(entry, blocks), wanted)
    need_out[...] = wanted
    k_copy.wait()
    v_copy.wait()
    for c in range(CHUNKS):
        whole = k_all if c < CHUNKS // 2 else v_all
        start = (c % (CHUNKS // 2)) * chunk_rows
        chunk_out[c] = whole[0, start : start + chunk_rows]
    pl.semaphore_wait(barrier, devices - 1)

    def need_copy(k):
        return pltpu.make_async_remote_copy(
            need_out, need_in.at[k], send_need.at[k], recv_need.at[k], device_id={"seq": peer(k)}
        )

    def chunk_copy(k):
        return pltpu.make_async_remote_copy(
            chunk_out.at[lax.rem(peer(k), CHUNKS)],
            chunk_in.at[me],
            send_chunk.at[k],
            recv_chunk.at[k],
            device_id={"seq": peer(k)},
        )

    def reg_copy(k):
        return pltpu.make_async_remote_copy(
            reg_out, reg_in.at[me], send_reg.at[k], recv_reg.at[k], device_id={"seq": peer(k)}
        )

    def x_copy(k, g):
        return pltpu.make_async_remote_copy(
            x_out.at[k, g], x_in.at[k, g], send_x.at[k, g], recv_x.at[k, g], device_id={"seq": peer(k)}
        )

    order = list(reversed(peers))
    for k in order:
        need_copy(k).start()
    for k in order:
        chunk_copy(k).start()
    chunk_in[me] = chunk_out[lax.rem(me, CHUNKS)]

    stages = stage_list(devices)

    for k in peers:
        chunk_copy(k).wait_recv()
    mine = chunk_in[owner_ref[0]]
    reg_out[...] = mine
    reg_in[me] = mine
    for k in order:
        reg_copy(k).start()
    for k in peers:
        need_copy(k).wait_recv()
    for group_of in stages:
        for k in group_of:
            row = need_in[k]
            pick = jnp.sum(jnp.where(lane[:1] == me, row[:1], 0))
            k_block = k_all[pick]
            v_block = v_all[pick]
            for g in range(KEY_VALUE_HEADS):
                columns = slice(g * HEAD_SIZE, (g + 1) * HEAD_SIZE)
                x_out[k, g, :rows] = k_block[:, columns]
                x_out[k, g, rows:] = v_block[:, columns]
        for g in range(KEY_VALUE_HEADS):
            for k in group_of:
                x_copy(k, g).start()

    for b in range(blocks):
        count = counts_ref[b]
        for k in peers:
            source = peer(k)
            seen = jnp.int32(0)
            for t in range(slots):
                entry = lists_ref[b, t]
                hit = jnp.logical_and(lax.div(entry, blocks) == source, t < count)
                seen = jnp.where(hit, 1, seen)
            bias[b, k] = jnp.where(seen == 1, 0.0, hidden)

    def attend(b, g, keys, values, masks, first, last):
        index = g * blocks + b
        row_span = pl.ds(pl.multiple_of(b * rows, rows), rows)
        ones = jnp.ones(values.shape, values.dtype)
        wide = jnp.concatenate([values, ones], axis=1)
        columns = [
            pl.ds(pl.multiple_of((g * group + h) * HEAD_SIZE, HEAD_SIZE), HEAD_SIZE)
            for h in range(group)
        ]
        copies = masks.shape[0] // rows
        repeat = keys.shape[0] // 128

        def scored(part):
            query = jnp.concatenate([q_all[row_span, columns[h]] for h in part], axis=0)
            return lax.dot_general(
                query, keys, (((1,), (1,)), ((), ())), preferred_element_type=jnp.float32
            )

        parts = [list(range(group))[i : i + 4] for i in range(0, group, 4)]
        ahead = [scored(part) for part in parts[:1]]
        for step, part in enumerate(parts):
            if step + 1 < len(parts):
                ahead.append(scored(parts[step + 1]))
            scores = ahead[step]
            here = pl.ds(part[0] * rows, len(part) * rows)
            tall = jnp.concatenate([masks] * len(part), axis=0) if copies else masks
            scores = scores * score_gain + tall
            best = jnp.max(scores, axis=1, keepdims=True)
            if first:
                best = jnp.broadcast_to(best, (len(part) * rows, 128))
            else:
                before = top[index, here]
                best = jnp.maximum(before, best)
            spread = jnp.concatenate([best] * repeat, axis=1) if repeat > 1 else best
            weights = jnp.exp2(scores - spread).astype(jnp.bfloat16)
            product = jnp.dot(weights, wide, preferred_element_type=jnp.float32)
            if not first:
                scale = jnp.exp2(before - best)
                product = product + acc[index, here] * jnp.concatenate([scale, scale], axis=1)
            if last:
                merged = product[:, :HEAD_SIZE] / product[:, HEAD_SIZE:]
                merged = merged.astype(out_ref.dtype)
                for n, h in enumerate(part):
                    out_ref[row_span, columns[h]] = merged[n * rows : (n + 1) * rows]
            else:
                acc[index, here] = product
                top[index, here] = best

    def own_step(i, carry):
        b = i // KEY_VALUE_HEADS
        g = lax.rem(i, KEY_VALUE_HEADS)

        @pl.when(g == 0)
        def _():
            q_copy(b).wait()

        column = pl.ds(pl.multiple_of(g * HEAD_SIZE, HEAD_SIZE), HEAD_SIZE)
        below = lax.broadcasted_iota(jnp.int32, (rows, rows), 1) <= lax.broadcasted_iota(
            jnp.int32, (rows, rows), 0
        )
        shut = jnp.where(image_ref[b] == 1, 0.0, hidden)
        masks = jnp.where(below, 0.0, shut)
        attend(b, g, k_all[b, :, column], v_all[b, :, column], masks, True, False)
        return carry

    lax.fori_loop(0, blocks * KEY_VALUE_HEADS, own_step, 0)

    for k in peers:
        reg_copy(k).wait_recv()

    half = CHUNKS // 2

    def far_step(i, carry, stage):
        g = i // blocks
        b = lax.rem(i, blocks)

        @pl.when(b == 0)
        def _():
            for k in stage:
                x_copy(k, g).wait_recv()

        keys = [x_in[k, g, :rows] for k in stage]
        values = [x_in[k, g, rows:] for k in stage]
        masks = [jnp.full((1, rows), bias[b, k]) for k in stage]
        if stage == stages[0]:
            column = pl.ds(pl.multiple_of(g * HEAD_SIZE, HEAD_SIZE), HEAD_SIZE)
            fill = jnp.zeros((128 - REG, HEAD_SIZE), jnp.bfloat16)
            keys += [reg_in[pl.ds(0, half), :, column].reshape(REG, HEAD_SIZE), fill]
            values += [reg_in[pl.ds(half, half), :, column].reshape(REG, HEAD_SIZE), fill]
            side = lax.broadcasted_iota(jnp.int32, (1, 128), 1)
            masks += [jnp.where(side < REG, 0.0, hidden)]
        keys = jnp.concatenate(keys, axis=0)
        values = jnp.concatenate(values, axis=0)
        masks = jnp.concatenate(masks, axis=1)
        attend(b, g, keys, values, masks, False, stage == stages[-1])
        return carry

    for stage in stages:
        lax.fori_loop(
            0, blocks * KEY_VALUE_HEADS, functools.partial(far_step, stage=stage), 0
        )

    for k in peers:
        need_copy(k).wait_send()
        chunk_copy(k).wait_send()
        reg_copy(k).wait_send()
        for g in range(KEY_VALUE_HEADS):
            x_copy(k, g).wait_send()


def per_device(queries, keys, values, reg_owner, block_lists, list_counts, image_blocks):
    devices = lax.axis_size("seq")
    tokens, width = queries.shape[1:]
    kv_width = keys.shape[2]
    blocks = block_lists.shape[1]
    rows = tokens // blocks
    chunk_rows = 2 * REG // CHUNKS
    group_rows = width // kv_width * rows
    bf = jnp.bfloat16
    dma = pltpu.SemaphoreType.DMA
    smem = pl.BlockSpec(memory_space=pltpu.SMEM)
    anywhere = pl.BlockSpec(memory_space=pl.ANY)
    out = pl.pallas_call(
        functools.partial(kernel, devices),
        out_shape=jax.ShapeDtypeStruct((tokens, width), bf),
        in_specs=[smem] * 4 + [anywhere] * 3,
        out_specs=pl.BlockSpec(memory_space=pltpu.VMEM),
        scratch_shapes=[
            pltpu.VMEM((tokens, width), bf),
            pltpu.VMEM((blocks, rows, kv_width), bf),
            pltpu.VMEM((blocks, rows, kv_width), bf),
            pltpu.VMEM((8, 128), jnp.int32),
            pltpu.VMEM((devices, 8, 128), jnp.int32),
            pltpu.VMEM((CHUNKS, chunk_rows, kv_width), bf),
            pltpu.VMEM((devices, chunk_rows, kv_width), bf),
            pltpu.VMEM((chunk_rows, kv_width), bf),
            pltpu.VMEM((devices, chunk_rows, kv_width), bf),
            pltpu.VMEM((devices, KEY_VALUE_HEADS, 2 * rows, HEAD_SIZE), bf),
            pltpu.VMEM((devices, KEY_VALUE_HEADS, 2 * rows, HEAD_SIZE), bf),
            pltpu.VMEM((blocks * KEY_VALUE_HEADS, group_rows, 2 * HEAD_SIZE), jnp.float32),
            pltpu.VMEM((blocks * KEY_VALUE_HEADS, group_rows, 128), jnp.float32),
            pltpu.SMEM((blocks, devices), jnp.float32),
            dma((2,)),
            dma((blocks,)),
            dma((devices,)),
            dma((devices,)),
            dma((devices,)),
            dma((devices,)),
            dma((devices,)),
            dma((devices,)),
            dma((devices, KEY_VALUE_HEADS)),
            dma((devices, KEY_VALUE_HEADS)),
        ],
        compiler_params=pltpu.CompilerParams(
            collective_id=0, has_side_effects=True, vmem_limit_bytes=38 * 1024 * 1024 + devices * kv_width * rows * 8
        ),
    )(
        block_lists[0],
        list_counts[0],
        image_blocks[0],
        reg_owner,
        queries[0],
        keys.reshape(blocks, rows, kv_width),
        values.reshape(blocks, rows, kv_width),
    )
    return out[None]


def solution(mesh):
    placed = (
        P("samp", "seq", None),
        P("samp", "seq", None),
        P("samp", "seq", None),
        P("samp"),
        P("samp", "seq", None),
        P("samp", "seq"),
        P("samp", "seq"),
    )
    return jax.shard_map(
        per_device, mesh=mesh, in_specs=placed, out_specs=P("samp", "seq", None), check_vma=False
    )
```
